256 devices in a mesh: region: 32 (over x, z), member: 8 (over y, core).
Axes of the slice: x: 4, y: 4, z: 8, core: 2. Of those that a mesh axis runs over, the one named last changes fastest.
Arguments:
- ensemble: bfloat16 [80, 524288], P('member', 'region'), may hold values from -6 to 6
- obs_value: float32 [8192, 128], P(('region', 'member')), may hold values from -8 to 8
- obs_var: float32 [8192, 128], P(('region', 'member')), may hold values from 0.1 to 1
- obs_point: int32 [8192, 128], P(('region', 'member')), may hold values from 0 to 16383
- owned_blocks: int32 [4096], P('region'), may hold values from 0 to 4095, each once
- infl_mean: float32 [4096], replicated, may hold values from 0.6 to 1.6
- infl_var: float32 [4096], replicated, may hold values from 0.0001 to 0.1
Outputs:
- inflated: bfloat16 [80, 524288], P('member', 'region')
- infl_post: float32 [4096], P(('region', 'member'))
The draws below stay inside these ranges and needn't reach their ends.
Inputs may be any that keep to these rules, and one draw needn't show every extreme that they name: `obs_point`: index among the 16384 points of the observation's region; the observation belongs to the block of that point's slot. `owned_blocks`: every block id appears exactly once.
All inputs are finite; a program needn't handle non-finite values.
Results may differ from the reference program's by a relative error of at most 0.001.
Values sent between devices are 32-bit elements; how exact they have to be, the bound alone decides.
A program may use at most 64 MiB of HBM per device.

```python
import math
import jax
import jax.numpy as jnp
from jax import lax

PTS_DEV = 16384
OBS_DEV = 4096
MEMBERS = 80
PTS = 524288
BLOCKS = 4096
SPAN = 128
OBS_ROWS = 8192
N_MEMBER = 8


def with_ends(values, rng, low, top_value):
    shape = values.shape
    index_at = [jax.random.randint(jax.random.fold_in(rng, axis), (), 0, shape[axis]) for axis in range(len(shape))]
    values = values.at[tuple(index_at)].set(low)
    longest = shape.index(max(shape))
    index_at[longest] = (index_at[longest] + 1) % shape[longest]
    return values.at[tuple(index_at)].set(top_value)


def block_scale(rng, shape, shards, least, largest):
    def one(position, shards_of):
        heights = jax.random.uniform(jax.random.fold_in(jax.random.fold_in(rng, 6), position), (shards_of,), jnp.float32, least / len(shards), largest / len(shards))
        return jnp.repeat(jnp.exp(heights), shape[position] // shards_of).reshape((-1,) + (1,) * (len(shape) - position - 1))

    loudness = one(*shards[0])
    for cut in shards[1:]:
        loudness = loudness * one(*cut)
    return loudness


def scatter_about(rng, extent, width, reach, shards=(), kind=jnp.bfloat16):
    gain = block_scale(rng, extent, shards, -0.22, 0.18) if shards else 1.0
    result = jax.random.normal(rng, extent, jnp.float32) * width * gain
    return jnp.minimum(jnp.maximum(result, -reach), reach).astype(kind)


def setup_inputs(seed: int = 0) -> dict:
    arg_keys = jax.random.split(jax.random.key(seed), 8)
    return {
        "ensemble": scatter_about(arg_keys[0], (MEMBERS, PTS), 1.0, 6.0, ((0, 8), (1, 32))),
        "obs_value": scatter_about(arg_keys[1], (OBS_ROWS, 128), 1.3, 8.0, ((0, 256),), jnp.float32),
        "obs_var": jnp.clip(jnp.exp(math.log(1.0) - 2.3025851 * jax.random.uniform(arg_keys[2], (OBS_ROWS, 128), jnp.float32) ** block_scale(arg_keys[2], (OBS_ROWS, 128), ((0, 256),), -0.2, 0.2)), 0.1, 1.0),
        "obs_point": with_ends(jax.random.randint(arg_keys[3], (OBS_ROWS, 128), 0, PTS_DEV), jax.random.fold_in(arg_keys[3], 1), 0, PTS_DEV - 1).astype(jnp.int32),
        "owned_blocks": jax.random.permutation(arg_keys[4], BLOCKS).astype(jnp.int32),
        "infl_mean": jnp.clip(jax.random.uniform(arg_keys[5], (BLOCKS,), jnp.float32, 0.6, 1.6), 0.6, 1.6),
        "infl_var": jnp.clip(jnp.exp(jax.random.uniform(arg_keys[6], (BLOCKS,), jnp.float32, math.log(0.0001), math.log(0.1))), 0.0001, 0.1),
    }


def posterior(sums, prior_mean, prior_var):
    innov_sum = sums[0]
    spread_sum = sums[1]
    error_sum = sums[2]
    spread_spread = sums[3]
    spread_error = sums[4]
    error_error = sums[5]
    weight_var = 2.0 * prior_mean * prior_mean * (1.0 + spread_spread) + 4.0 * prior_mean * spread_error + 2.0 * error_error
    value = (prior_mean * weight_var + prior_var * spread_sum * (innov_sum - error_sum)) / (weight_var + prior_var * spread_sum * spread_sum)
    return jnp.maximum(value, 1.0)

def reference(ensemble, obs_value, obs_var, obs_point, owned_blocks, infl_mean, infl_var):
    wide = ensemble.astype(jnp.float32)
    point_total = lax.optimization_barrier(jnp.sum(wide, 0))
    point_square = lax.optimization_barrier(jnp.sum(wide * wide, 0))
    point_mean = point_total / MEMBERS
    row_region = jnp.arange(OBS_ROWS, dtype=jnp.int32) // (OBS_DEV // 128 * N_MEMBER)
    global_point = (row_region[:, None] * PTS_DEV + obs_point).reshape(-1).astype(jnp.int32)
    at_mean = point_mean[global_point]
    at_square = point_square[global_point]
    spread = (at_square - MEMBERS * at_mean * at_mean) / (MEMBERS - 1)
    innovation = obs_value.reshape(-1) - at_mean
    errors = obs_var.reshape(-1)
    obs_blk = owned_blocks[(global_point // SPAN).astype(jnp.int32)].astype(jnp.int32)
    columns = jnp.stack([innovation * innovation, spread, errors, spread * spread, spread * errors, errors * errors], 1)
    sums = jax.ops.segment_sum(columns, obs_blk, num_segments=BLOCKS)
    infl_post = posterior(sums.T, infl_mean, infl_var)
    point_lambda = jnp.repeat(infl_post[owned_blocks], SPAN)
    inflated = (point_mean + jnp.sqrt(point_lambda) * (wide - point_mean)).astype(jnp.bfloat16)
    return (inflated, infl_post)
```

```python
import functools

import jax
import jax.numpy as jnp
from jax import lax
from jax.experimental import pallas as pl
from jax.experimental.pallas import tpu as pltpu
from jax.sharding import PartitionSpec as P

LANES = 128
MESH = pl.DeviceIdType.MESH
F32 = jnp.float32
BF16 = jnp.bfloat16
NT = (((1,), (1,)), ((), ()))


def split(value, parts):
    terms = []
    for _ in range(parts):
        term = value.astype(BF16).astype(F32)
        terms.append(term)
        value = value - term
    return terms


def scatter(value_ref, var_ref, point_ref, acc, row_acc, half):
    rows = point_ref.shape[0]
    step = 8
    low_ids = lax.broadcasted_iota(jnp.int32, (half, LANES), 0)
    col_ids = lax.broadcasted_iota(jnp.int32, (2 * LANES, LANES), 0)
    slot_ids = lax.broadcasted_iota(jnp.int32, (2 * half, LANES), 0)

    def chunk(first):
        point = point_ref[pl.ds(first, step), :]
        slot = point >> 7
        upper = (slot >= half).astype(jnp.int32)
        low = slot - half * upper
        col = (point & (LANES - 1)) + LANES * upper
        y = split(value_ref[pl.ds(first, step), :], 2)
        exact = y[0] + y[1]
        raw = var_ref[pl.ds(first, step), :]
        v = split(raw, 2)
        terms = [jnp.ones_like(raw)] + y + v
        row_terms = v + split(raw * raw, 3) + split(exact * exact, 3)
        left, right, hots = [], [], []
        row_left = []
        for r in range(step):
            here = slice(r, r + 1)
            hot = (low_ids == low[here, :]).astype(F32).astype(BF16)
            blocks = []
            for term in terms:
                wide = jnp.broadcast_to(term[here, :], (16, LANES)).astype(BF16)
                blocks.append(hot * jnp.concatenate([wide] * (half // 16), 0))
            left.append(jnp.concatenate(blocks, 0))
            right.append((col_ids == col[here, :]).astype(F32).astype(BF16))
            hots.append((slot_ids == slot[here, :]).astype(F32).astype(BF16))
            row_left.append(jnp.concatenate([term[here, :] for term in row_terms], 0))
        points = lax.dot_general(
            jnp.concatenate(left, 1), jnp.concatenate(right, 1), NT, preferred_element_type=F32
        )
        by_slot = lax.dot_general(
            jnp.concatenate(row_left, 1).astype(BF16), jnp.concatenate(hots, 1), NT,
            preferred_element_type=F32,
        )
        return points, by_slot

    def add(i):
        points, by_slot = chunk(pl.multiple_of(i * step, step))
        acc[...] += points
        row_acc[...] += by_slot

    points, by_slot = chunk(0)
    acc[...] = points
    row_acc[...] = by_slot
    pl.loop(1, rows // step)(add)


def kernel(
    n_region, n_member, members,
    ens_hbm, value_hbm, var_hbm, point_hbm, owned_hbm, pmean_hbm, pvar_hbm,
    out_ref, post_ref,
    ens, value, var, point, owned, pmean, pvar,
    part, rs_recv, means, factors, acc, row_acc, place, place_recv,
    in_sem, send_sem, got_sem,
):
    region = lax.axis_index("region")
    me = lax.axis_index("member")
    slots = owned.shape[1]
    own = slots // n_member
    half = slots // 2
    devices = n_region * n_member
    flat = region * n_member + me

    pairs = (
        (ens_hbm, ens), (point_hbm, point), (value_hbm, value), (var_hbm, var),
        (owned_hbm, owned), (pmean_hbm, pmean), (pvar_hbm, pvar),
    )
    loads = [pltpu.make_async_copy(s, d, in_sem.at[i]) for i, (s, d) in enumerate(pairs)]
    for load in loads:
        load.start()

    member_at = [me] + [lax.rem(me + j, n_member) for j in range(1, n_member)]
    region_at = [region] + [lax.rem(region + k, n_region) for k in range(1, n_region)]
    barrier = pltpu.get_barrier_semaphore()
    for j in range(1, n_member):
        pl.semaphore_signal(barrier, inc=1, device_id=(region, member_at[j]), device_id_type=MESH)
    for k in range(1, n_region):
        pl.semaphore_signal(barrier, inc=1, device_id=(region_at[k], me), device_id_type=MESH)
    loads[0].wait()

    @pl.loop(0, n_member)
    def _(k):
        @pl.loop(0, own, unroll=8)
        def _(r):
            start = pl.multiple_of((k * own + r) * LANES, LANES)
            wide = ens[:, pl.ds(start, LANES)].astype(F32)
            part[k, pl.ds(r, 1), :] = jnp.sum(wide, 0, keepdims=True)
            part[k, pl.ds(own + r, 1), :] = jnp.sum(wide * wide, 0, keepdims=True)

    pl.semaphore_wait(barrier, n_member - 1 + n_region - 1)

    def send(src, dst, phase, coords):
        pltpu.make_async_remote_copy(
            src, dst, send_sem.at[phase], got_sem.at[phase], device_id=coords, device_id_type=MESH
        ).start()

    def drain(ref, sem):
        pltpu.make_async_copy(ref, ref, sem).wait()

    def reduce_copies(first, count, phase):
        for i in range(1, n_member):
            there = member_at[i]
            send(
                part.at[there, pl.ds(first, count), :], rs_recv.at[i, pl.ds(first, count), :],
                phase, (region, there),
            )

    reduce_copies(0, 2 * own, 0)
    for load in loads[1:]:
        load.wait()
    scatter(value, var, point, acc, row_acc, half)

    for index, (first, last) in enumerate(((0, 1), (1, 3), (3, 5))):
        both = acc[first * half : (first + 1) * half, :]
        for other in range(first + 1, last):
            both = both + acc[other * half : (other + 1) * half, :]
        table = jnp.concatenate([both[:, :LANES], both[:, LANES:]], 0)
        for k in range(n_member):
            part[k, (2 + index) * own : (3 + index) * own, :] = table[k * own : (k + 1) * own]
    sums = row_acc[...]
    rows = jnp.concatenate(
        [
            sums[0:1] + sums[1:2],
            sums[2:3] + sums[3:4] + sums[4:5],
            sums[5:6] + sums[6:7] + sums[7:8],
            jnp.zeros((5, slots), F32),
        ],
        0,
    )
    for k in range(n_member):
        part[k, 5 * own :, :] = rows

    reduce_copies(2 * own, 3 * own + 8, 1)

    block = owned[...]
    groups = pmean.shape[0]
    lane_hot = (
        lax.broadcasted_iota(jnp.int32, (LANES, slots), 0) == (block & (LANES - 1))
    ).astype(F32).astype(BF16)
    table = jnp.concatenate(split(pmean[...], 3) + split(pvar[...], 3), 0).astype(BF16)
    picked = jnp.dot(table, lane_hot, preferred_element_type=F32)
    in_group = lax.broadcasted_iota(jnp.int32, (groups, slots), 0) == (block >> 7)

    def pick(first):
        total = picked[first * groups : (first + 1) * groups]
        for i in (1, 2):
            total = total + picked[(first + i) * groups : (first + i + 1) * groups]
        return jnp.sum(jnp.where(in_group, total, 0.0), 0, keepdims=True)

    prior_mean, prior_var = pick(0), pick(3)
    share = groups * LANES // devices
    lane = lax.broadcasted_iota(jnp.int32, (1, slots), 1)
    target = lax.broadcasted_iota(jnp.int32, (devices, slots), 0) == jnp.where(
        lane // own == me, block // share, -1
    )
    spots = (
        lax.broadcasted_iota(jnp.int32, (LANES, slots), 0) == lax.rem(block, share)
    ).astype(F32).astype(BF16)
    mine = lax.broadcasted_iota(jnp.int32, (own, slots), 1) == (
        lax.broadcasted_iota(jnp.int32, (own, slots), 0) + own * me
    )

    others = pl.ds(1, n_member - 1)
    drain(rs_recv.at[others, pl.ds(0, 2 * own), :], got_sem.at[0])

    def reduced(first, last):
        terms = [part[me, first:last, :]] + [rs_recv[i, first:last, :] for i in range(1, n_member)]
        while len(terms) > 1:
            terms = [a + b for a, b in zip(terms[::2], terms[1::2])]
        return terms[0]

    both = reduced(0, 2 * own)
    mean = both[:own] / members
    means[me] = mean
    for i in range(1, n_member):
        send(means.at[me], means.at[me], 2, (region, member_at[i]))
    spread = (both[own:] - members * mean * mean) / (members - 1)
    drain(rs_recv.at[others, pl.ds(2 * own, 3 * own + 8), :], got_sem.at[1])
    count = reduced(2 * own, 3 * own)
    y_sum = reduced(3 * own, 4 * own)
    v_sum = reduced(4 * own, 5 * own)
    by_slot = reduced(5 * own, 5 * own + 8)

    def to_row(table):
        column = jnp.sum(table, axis=1, keepdims=True)
        return jnp.sum(jnp.where(mine, column, 0.0), axis=0, keepdims=True)

    seen = count * spread
    so, soo = by_slot[0:1], by_slot[1:2]
    sd = by_slot[2:3] + to_row(mean * (count * mean - 2.0 * y_sum))
    sp, spp, spo = to_row(seen), to_row(seen * spread), to_row(v_sum * spread)
    weight = 2.0 * prior_mean * prior_mean * (1.0 + spp) + 4.0 * prior_mean * spo + 2.0 * soo
    post = jnp.maximum(
        (prior_mean * weight + prior_var * sp * (sd - so)) / (weight + prior_var * sp * sp), 1.0
    )

    sent = jnp.concatenate([jnp.where(target, term, 0.0) for term in split(post, 3)], 0)
    placed = lax.dot_general(sent.astype(BF16), spots, NT, preferred_element_type=F32)
    placed = placed[:devices] + placed[devices : 2 * devices] + placed[2 * devices :]
    for d in range(devices):
        place[d] = placed[d : d + 1]
    column = jnp.sum(jnp.where(mine, post, 0.0), axis=1, keepdims=True)
    factors[me] = jnp.broadcast_to(jnp.sqrt(column), (own, LANES))
    for k in sorted(range(n_region), key=lambda k: -min(k % 8, 8 - k % 8) - min(k // 8, 4 - k // 8)):
        for j in range(n_member):
            if k or j:
                send(
                    place.at[region_at[k] * n_member + member_at[j]], place_recv.at[k * n_member + j],
                    3, (region_at[k], member_at[j]),
                )
    for i in range(1, n_member):
        send(factors.at[me], factors.at[me], 4, (region, member_at[i]))
    drain(means.at[others], got_sem.at[2])
    drain(factors.at[others], got_sem.at[4])

    @pl.loop(0, n_member)
    def _(k):
        @pl.loop(0, own, unroll=8)
        def _(r):
            start = pl.multiple_of((k * own + r) * LANES, LANES)
            wide = ens[:, pl.ds(start, LANES)].astype(F32)
            at = means[k, pl.ds(r, 1), :]
            out_ref[:, pl.ds(start, LANES)] = (
                at + factors[k, pl.ds(r, 1), :] * (wide - at)
            ).astype(BF16)

    drain(rs_recv.at[others, pl.ds(0, 2 * own), :], send_sem.at[0])
    drain(rs_recv.at[others, pl.ds(2 * own, 3 * own + 8), :], send_sem.at[1])
    drain(means.at[others], send_sem.at[2])
    drain(factors.at[others], send_sem.at[4])
    rest = pl.ds(1, devices - 1)
    drain(place_recv.at[rest], got_sem.at[3])
    terms = [place[flat]] + [place_recv[i] for i in range(1, devices)]
    while len(terms) > 1:
        terms = [a + b for a, b in zip(terms[::2], terms[1::2])]
    post_ref[...] = terms[0][:, :share]
    drain(place_recv.at[rest], send_sem.at[3])


def body(n_region, n_member, ensemble, obs_value, obs_var, obs_point, owned, infl_mean, infl_var):
    members = ensemble.shape[0] * n_member
    slots = owned.shape[0]
    own = slots // n_member
    blocks = infl_mean.shape[0]
    devices = n_region * n_member
    share = blocks // devices
    owned = owned.reshape(1, slots)
    infl_mean = infl_mean.reshape(-1, LANES)
    infl_var = infl_var.reshape(-1, LANES)
    operands = (ensemble, obs_value, obs_var, obs_point, owned, infl_mean, infl_var)
    dma = pltpu.SemaphoreType.DMA
    operands = tuple(pltpu.with_memory_space_constraint(x, pltpu.HBM) for x in operands)
    inflated, post = pl.pallas_call(
        functools.partial(kernel, n_region, n_member, members),
        out_shape=(
            jax.ShapeDtypeStruct(ensemble.shape, BF16),
            jax.ShapeDtypeStruct((1, share), F32),
        ),
        in_specs=[pl.BlockSpec(memory_space=pltpu.HBM)] * len(operands),
        out_specs=(
            pl.BlockSpec(memory_space=pltpu.VMEM),
            pl.BlockSpec(memory_space=pltpu.VMEM),
        ),
        scratch_shapes=[pltpu.VMEM(a.shape, a.dtype) for a in operands]
        + [
            pltpu.VMEM((n_member, 5 * own + 8, LANES), F32),
            pltpu.VMEM((n_member, 5 * own + 8, LANES), F32),
            pltpu.VMEM((n_member, own, LANES), F32),
            pltpu.VMEM((n_member, own, LANES), F32),
            pltpu.VMEM((5 * (slots // 2), 2 * LANES), F32),
            pltpu.VMEM((8, slots), F32),
            pltpu.VMEM((devices, 1, LANES), F32),
            pltpu.VMEM((devices, 1, LANES), F32),
            dma((len(operands),)),
            dma((5,)), dma((5,)),
        ],
        compiler_params=pltpu.CompilerParams(collective_id=0, has_side_effects=True, vmem_limit_bytes=12*2**20),
    )(*operands)
    return inflated, post.reshape(share)


def solution(mesh):
    placed = (
        P("member", "region"),
        P(("region", "member"), None),
        P(("region", "member"), None),
        P(("region", "member"), None),
        P("region"),
        P(),
        P(),
    )
    return jax.shard_map(
        functools.partial(body, mesh.shape["region"], mesh.shape["member"]),
        mesh=mesh,
        in_specs=placed,
        out_specs=(P("member", "region"), P(("region", "member"))),
        check_vma=False,
    )
```
